32 devices in a mesh: dp: 1 (over z), ep: 32 (over y, x, core).
Axes of the slice: x: 4, y: 4, z: 1, core: 2. Of those that a mesh axis runs over, the one named last changes fastest.
The devices are a block of a 4x4x8 slice.
Arguments:
- x_in: bfloat16 [1024, 2048], P(('dp', 'ep'))
- k_cache: bfloat16 [1024, 32, 16, 128], P(('dp', 'ep'))
- v_cache: bfloat16 [1024, 32, 16, 128], P(('dp', 'ep'))
- cache_len: int32 [1024], P(('dp', 'ep'))
- topk_idx: int32 [1024, 8], P(('dp', 'ep'))
- ln_attn: bfloat16 [2048], replicated
- w_q: bfloat16 [2048, 2048], replicated
- w_k: bfloat16 [2048, 2048], replicated
- w_v: bfloat16 [2048, 2048], replicated
- q_norm: bfloat16 [128], replicated
- k_norm: bfloat16 [128], replicated
- w_o: bfloat16 [2048, 2048], replicated
- ln_moe: bfloat16 [2048], replicated
- w_router: bfloat16 [2048, 64], replicated
- w_gate: bfloat16 [64, 2048, 1024], P('ep')
- w_up: bfloat16 [64, 2048, 1024], P('ep')
- w_down: bfloat16 [64, 1024, 2048], P('ep')
Outputs:
- output 1: bfloat16 [1024, 2048], P(('dp', 'ep'))
- output 2: bfloat16 [1024, 32, 16, 128], P(('dp', 'ep'))
- output 3: bfloat16 [1024, 32, 16, 128], P(('dp', 'ep'))
All inputs are finite; a program needn't handle non-finite values.
Results may differ from the reference program's by a relative error of at most 0.0142719.
Values are sent between devices in bfloat16 or wider.
A program may use at most 768 MiB of HBM per device.

```python
import jax
import jax.numpy as jnp
import numpy as np
from jax import lax

HIDDEN = 2048
Q_HEADS = 16
KV_HEADS = 16
HEAD_DIM = 128
EXPERTS = 64
TOP_K = 8
EXPERT_FF = 1024
B_DEV = 32
CACHE_LEN = 32
EP_SIZE = 32
BATCH = B_DEV * EP_SIZE
E_LOCAL = EXPERTS // EP_SIZE
ROPE_BASE = 1000000.0
NORM_EPS = 1e-6


def draw_layout(len_key, route_key, local_key):
    pair_count = B_DEV * TOP_K
    cap_rows = min(B_DEV, 2 * pair_count // EP_SIZE)
    n_hot = EP_SIZE // TOP_K
    n_cold = EP_SIZE - n_hot
    rest_rows = pair_count - n_hot * cap_rows
    base_rows = rest_rows // n_cold
    extra_rows = rest_rows - base_rows * n_cold
    row_counts = [cap_rows] * n_hot + [base_rows + 1] * extra_rows + [base_rows] * (n_cold - extra_rows)
    rank_table = np.repeat(np.arange(EP_SIZE), row_counts).reshape(TOP_K, B_DEV).T
    dev_keys = jax.random.split(route_key, EP_SIZE + 1)
    dev_perm = jax.random.permutation(dev_keys[0], EP_SIZE)
    row_perms = jax.vmap(lambda key_one: jax.random.permutation(key_one, B_DEV))(dev_keys[1:])
    dev_table = dev_perm[jnp.asarray(rank_table)]
    dev_all = dev_table[row_perms]
    local_ids = jax.random.randint(local_key, (EP_SIZE, B_DEV, TOP_K), 0, E_LOCAL)
    topk_idx = (dev_all * E_LOCAL + local_ids).reshape(BATCH, TOP_K).astype(jnp.int32)
    len_keys = jax.random.split(len_key, 3)
    shard_top = jax.random.randint(len_keys[0], (EP_SIZE, 1), CACHE_LEN // 4, CACHE_LEN)
    len_draw = jax.random.randint(len_keys[1], (EP_SIZE, B_DEV), 1, shard_top).reshape(BATCH)
    longest = jax.random.randint(len_keys[2], (), 0, BATCH)
    cache_len = jnp.where(jnp.arange(BATCH) == longest, CACHE_LEN - 1, len_draw).astype(jnp.int32)
    return cache_len, topk_idx


def setup_inputs(seed: int = 0, part: int = 0) -> dict:
    base_key = jax.random.key(seed)
    part_keys = jax.random.split(jax.random.fold_in(base_key, part), 6)
    shared_keys = jax.random.split(base_key, 14)
    q_width = Q_HEADS * HEAD_DIM
    kv_width = KV_HEADS * HEAD_DIM

    def normal_of(rand_key, arr_shape, scale_mul):
        return jax.random.normal(rand_key, arr_shape, jnp.float32) * scale_mul

    cache_len, topk_idx = draw_layout(part_keys[3], part_keys[4], part_keys[5])
    cache_shape = (BATCH, CACHE_LEN, KV_HEADS, HEAD_DIM)
    return {
        'x_in': normal_of(part_keys[0], (BATCH, HIDDEN), 1.0).astype(jnp.bfloat16),
        'k_cache': normal_of(part_keys[1], cache_shape, 1.5).astype(jnp.bfloat16),
        'v_cache': normal_of(part_keys[2], cache_shape, 1.0).astype(jnp.bfloat16),
        'cache_len': cache_len,
        'topk_idx': topk_idx,
        'ln_attn': (1.0 + normal_of(shared_keys[0], (HIDDEN,), 0.3)).astype(jnp.bfloat16),
        'w_q': normal_of(shared_keys[1], (HIDDEN, q_width), HIDDEN ** -0.5).astype(jnp.bfloat16),
        'w_k': normal_of(shared_keys[2], (HIDDEN, kv_width), HIDDEN ** -0.5).astype(jnp.bfloat16),
        'w_v': normal_of(shared_keys[3], (HIDDEN, kv_width), HIDDEN ** -0.5).astype(jnp.bfloat16),
        'q_norm': (2.0 + normal_of(shared_keys[4], (HEAD_DIM,), 0.4)).astype(jnp.bfloat16),
        'k_norm': (2.0 + normal_of(shared_keys[5], (HEAD_DIM,), 0.4)).astype(jnp.bfloat16),
        'w_o': normal_of(shared_keys[6], (q_width, HIDDEN), q_width ** -0.5).astype(jnp.bfloat16),
        'ln_moe': (1.0 + normal_of(shared_keys[7], (HIDDEN,), 0.3)).astype(jnp.bfloat16),
        'w_router': normal_of(shared_keys[8], (HIDDEN, EXPERTS), 1.5 * HIDDEN ** -0.5).astype(jnp.bfloat16),
        'w_gate': normal_of(shared_keys[9], (EXPERTS, HIDDEN, EXPERT_FF), HIDDEN ** -0.5).astype(jnp.bfloat16),
        'w_up': normal_of(shared_keys[10], (EXPERTS, HIDDEN, EXPERT_FF), HIDDEN ** -0.5).astype(jnp.bfloat16),
        'w_down': normal_of(shared_keys[11], (EXPERTS, EXPERT_FF, HIDDEN), 3.0 * EXPERT_FF ** -0.5).astype(jnp.bfloat16),
    }


def norm_scale(values, gain_vec):
    return values * lax.rsqrt(jnp.mean(values * values, axis=-1, keepdims=True) + NORM_EPS) * gain_vec.astype(jnp.float32)


def rotate_halves(values, positions):
    half_dim = values.shape[-1] // 2
    freq_vec = ROPE_BASE ** (-jnp.arange(half_dim, dtype=jnp.float32) * 2.0 / values.shape[-1])
    angles = positions.astype(jnp.float32)[:, None, None] * freq_vec
    cosine = jnp.cos(angles)
    sine_val = jnp.sin(angles)
    lo_half = values[..., :half_dim]
    hi_half = values[..., half_dim:]
    return jnp.concatenate([lo_half * cosine - hi_half * sine_val, hi_half * cosine + lo_half * sine_val], axis=-1)


def reference(x_in, k_cache, v_cache, cache_len, topk_idx, ln_attn, w_q, w_k, w_v, q_norm, k_norm, w_o, ln_moe, w_router, w_gate, w_up, w_down):
    resid_in = x_in.astype(jnp.float32)
    normed = norm_scale(resid_in, ln_attn).astype(jnp.bfloat16)
    q_proj = jnp.dot(normed, w_q, preferred_element_type=jnp.float32).reshape(BATCH, Q_HEADS, HEAD_DIM)
    k_proj = jnp.dot(normed, w_k, preferred_element_type=jnp.float32).reshape(BATCH, KV_HEADS, HEAD_DIM)
    v_new = jnp.dot(normed, w_v, preferred_element_type=jnp.float32).astype(jnp.bfloat16).reshape(BATCH, KV_HEADS, HEAD_DIM)
    q_rot = rotate_halves(norm_scale(q_proj, q_norm), cache_len).astype(jnp.bfloat16)
    k_new = rotate_halves(norm_scale(k_proj, k_norm), cache_len).astype(jnp.bfloat16)
    slot_ids = jnp.arange(CACHE_LEN)
    is_new = slot_ids[None, :, None, None] == cache_len[:, None, None, None]
    k_full = jnp.where(is_new, k_new[:, None], k_cache)
    v_full = jnp.where(is_new, v_new[:, None], v_cache)

    def one_token(args_tok):
        q_tok, k_tok, v_tok, len_tok = args_tok
        q_grp = q_tok.reshape(KV_HEADS, Q_HEADS // KV_HEADS, HEAD_DIM).astype(jnp.float32)
        scores = jnp.einsum('grd,sgd->grs', q_grp, k_tok.astype(jnp.float32)) * HEAD_DIM ** -0.5
        scores = jnp.where(slot_ids <= len_tok, scores, -1e30)
        attn_prob = jax.nn.softmax(scores, axis=-1).astype(jnp.bfloat16)
        mixed = jnp.einsum('grs,sgd->grd', attn_prob.astype(jnp.float32), v_tok.astype(jnp.float32))
        return mixed.astype(jnp.bfloat16).reshape(Q_HEADS * HEAD_DIM)

    attn_out = lax.map(one_token, (q_rot, k_full, v_full, cache_len))
    x_mid = (resid_in + jnp.dot(attn_out, w_o, preferred_element_type=jnp.float32)).astype(jnp.bfloat16)
    resid_mid = x_mid.astype(jnp.float32)
    h_moe = norm_scale(resid_mid, ln_moe).astype(jnp.bfloat16)
    logits = jnp.dot(h_moe, w_router, preferred_element_type=jnp.float32)
    route_prob = jax.nn.softmax(logits, axis=-1)
    picked = jnp.take_along_axis(route_prob, topk_idx, axis=1)
    gate_wts = picked / jnp.sum(picked, axis=1, keepdims=True)
    tok_rows = jnp.repeat(h_moe, TOP_K, axis=0)

    def one_pair(args_pair):
        row_vec, expert = args_pair
        row_mat = row_vec[None, :]
        gate_act = jnp.dot(row_mat, w_gate[expert], preferred_element_type=jnp.float32)
        up_act = jnp.dot(row_mat, w_up[expert], preferred_element_type=jnp.float32)
        hidden_act = (jax.nn.silu(gate_act) * up_act).astype(jnp.bfloat16)
        return jnp.dot(hidden_act, w_down[expert], preferred_element_type=jnp.float32).astype(jnp.bfloat16)[0]

    expert_out = lax.map(one_pair, (tok_rows, topk_idx.reshape(BATCH * TOP_K)))
    moe_out = jnp.sum(expert_out.reshape(BATCH, TOP_K, HIDDEN).astype(jnp.float32) * gate_wts[:, :, None], axis=1)
    x_out = (resid_mid + moe_out).astype(jnp.bfloat16)
    return x_out, k_full, v_full
```

```python
import functools

import jax
import jax.numpy as jnp
from jax import lax
from jax.experimental import pallas as pl
from jax.experimental.pallas import tpu as pltpu
from jax.sharding import PartitionSpec as P

ROPE_BASE = 1000000.0
NORM_EPS = 1e-6
NEG = -1e30
RING = 4
CORES = 2
MESH = pl.DeviceIdType.MESH
F32 = jnp.float32
BF16 = jnp.bfloat16


def iota(shape, axis):
    return lax.broadcasted_iota(jnp.int32, shape, axis)


def split3(value):
    top = value.astype(BF16)
    rest = value - top.astype(F32)
    mid = rest.astype(BF16)
    low = (rest - mid.astype(F32)).astype(BF16)
    return top, mid, low


def dot32(lhs, rhs):
    return jnp.dot(lhs, rhs, preferred_element_type=F32)


def rms_rows(values, gain):
    return values * lax.rsqrt(jnp.mean(values * values, axis=-1, keepdims=True) + NORM_EPS) * gain


def route_rows(h_moe, topk, w_router, x_pos):
    rows, top_k = topk.shape
    experts = w_router.shape[1]
    e_local = experts // (RING * RING * CORES)
    devs = RING * RING * CORES
    seats = 2 * rows * top_k // devs
    logits = dot32(h_moe, w_router)
    expert_ids = iota((rows, experts), 1)
    hit = jnp.zeros((rows, experts), F32)
    for k in range(top_k):
        hit = hit + jnp.where(topk[:, k:k + 1] == expert_ids, 1.0, 0.0)
    chosen = hit > 0.5
    peak = jnp.max(jnp.where(chosen, logits, NEG), axis=1, keepdims=True)
    raw = jnp.where(chosen, jnp.exp(jnp.where(chosen, logits, peak) - peak), 0.0)
    gates = raw / jnp.sum(raw, axis=1, keepdims=True)
    hit_b = hit.astype(BF16)
    before = jnp.where(iota((rows, rows), 1) < iota((rows, rows), 0), 1.0, 0.0).astype(BF16)
    parts = split3(gates)
    lanes = devs * seats
    out = []
    for by_row in (True, False):
        lane_e = iota((experts, lanes), 1) // seats
        if by_row:
            lane_dev = lane_e
        else:
            lane_dev = (lane_e % (RING * CORES)) // CORES * (RING * CORES) + lane_e // (RING * CORES) * CORES + lane_e % CORES
        spread = jnp.where(iota((experts, lanes), 0) // e_local == lane_dev, 1.0, 0.0).astype(BF16)
        hit_l = dot32(hit_b, spread)
        rank_l = dot32(before, hit_l.astype(BF16))
        gate_l = dot32(parts[0], spread) + dot32(parts[1], spread) + dot32(parts[2], spread)
        seat_l = (iota((rows, lanes), 1) % seats).astype(F32)
        out.append(jnp.where(hit_l > 0.5, jnp.where(rank_l == seat_l, gate_l, 0.0), 0.0))
    place = jnp.where(iota((rows, 128), 1) == x_pos * rows + iota((rows, 128), 0), 1.0, 0.0).astype(BF16)
    marks = lax.dot_general((topk + 1).astype(F32).astype(BF16), place, (((0,), (0,)), ((), ())), preferred_element_type=F32)
    return out[0], out[1], marks


def norm_scale(values, gain_vec):
    return values * lax.rsqrt(jnp.mean(values * values, axis=-1, keepdims=True) + NORM_EPS) * gain_vec.astype(jnp.float32)


def rotate_halves(values, positions):
    half_dim = values.shape[-1] // 2
    freq_vec = ROPE_BASE ** (-jnp.arange(half_dim, dtype=jnp.float32) * 2.0 / values.shape[-1])
    angles = positions.astype(jnp.float32)[:, None, None] * freq_vec
    cosine = jnp.cos(angles)
    sine_val = jnp.sin(angles)
    lo_half = values[..., :half_dim]
    hi_half = values[..., half_dim:]
    return jnp.concatenate([lo_half * cosine - hi_half * sine_val, hi_half * cosine + lo_half * sine_val], axis=-1)


def attend_block(x_in, k_cache, v_cache, cache_len, ln_attn, w_q, w_k, w_v, q_norm, k_norm, w_o):
    n_batch, n_slots, kv_heads, head_dim = k_cache.shape
    q_heads = w_q.shape[1] // head_dim
    resid_in = x_in.astype(jnp.float32)
    normed = norm_scale(resid_in, ln_attn).astype(jnp.bfloat16)
    q_proj = jnp.dot(normed, w_q, preferred_element_type=jnp.float32).reshape(n_batch, q_heads, head_dim)
    k_proj = jnp.dot(normed, w_k, preferred_element_type=jnp.float32).reshape(n_batch, kv_heads, head_dim)
    v_new = jnp.dot(normed, w_v, preferred_element_type=jnp.float32).astype(jnp.bfloat16).reshape(n_batch, kv_heads, head_dim)
    q_rot = rotate_halves(norm_scale(q_proj, q_norm), cache_len).astype(jnp.bfloat16).reshape(n_batch, kv_heads, q_heads // kv_heads, head_dim)
    k_new = rotate_halves(norm_scale(k_proj, k_norm), cache_len).astype(jnp.bfloat16)
    len_col = cache_len[:, None, None, None]
    is_new = lax.broadcasted_iota(jnp.int32, (1, n_slots, 1, 1), 1) == len_col
    k_full = jnp.where(is_new, k_new[:, None], k_cache)
    v_full = jnp.where(is_new, v_new[:, None], v_cache)
    scores = jnp.einsum('bgrd,bsgd->bgrs', q_rot, k_full, preferred_element_type=jnp.float32) * head_dim ** -0.5
    seen = lax.broadcasted_iota(jnp.int32, (1, 1, 1, n_slots), 3) <= len_col
    attn_prob = jax.nn.softmax(jnp.where(seen, scores, -1e30), axis=-1).astype(jnp.bfloat16)
    attn_out = jnp.einsum('bgrs,bsgd->bgrd', attn_prob, v_full, preferred_element_type=jnp.float32).astype(jnp.bfloat16).reshape(n_batch, q_heads * head_dim)
    x_mid = (resid_in + jnp.dot(attn_out, w_o, preferred_element_type=jnp.float32)).astype(jnp.bfloat16)
    return x_mid, k_full, v_full


def route_kernel(x_mid, topk, ln_moe, w_router, h2, gate_a, gate_b, marks):
    h_moe = rms_rows(x_mid[...].astype(F32), ln_moe[...].astype(F32)).astype(BF16)
    h2[...] = h_moe
    x_pos = lax.axis_index('ep') // CORES % RING
    by_row, by_col, mark = route_rows(h_moe, topk[...], w_router[...], x_pos)
    for i in range(RING):
        gate_a[i] = by_row[:, i * 128:(i + 1) * 128]
        gate_b[i] = by_col[:, i * 128:(i + 1) * 128]
    marks[...] = mark


def route(x_mid, topk, ln_moe, w_router):
    rows, width = x_mid.shape
    return pl.pallas_call(
        route_kernel,
        out_shape=(jax.ShapeDtypeStruct((rows, width), BF16), jax.ShapeDtypeStruct((RING, rows, 128), F32), jax.ShapeDtypeStruct((RING, rows, 128), F32), jax.ShapeDtypeStruct((8, 128), F32)),
        name='route',
    )(x_mid, topk, ln_moe.reshape(1, width), w_router)


def exchange_kernel(h2, marks, gate_a, gate_b, x_mid, wg_hbm, wu_hbm, wd_hbm, out, hid, tok, gat_a, gat_b, wg, wu, wd, xs, ys, r1a, r1b, sa, sb, r2a, r2b,
                    w_sem, h_sem, t_sem, ga_sem, gb_sem, r1a_sem, r1b_sem, r2a_sem, r2b_sem, send_sem):
    rows, width = h2.shape
    half = width // 2
    seats = r1a.shape[2]
    ff = wg.shape[2]
    me = lax.axis_index('ep')
    c = me % CORES
    x = me // CORES % RING
    y = me // (CORES * RING)
    sends = []

    def dev(px, py, pc):
        return (py * RING + px) * CORES + pc

    def push(src, dst, sem, target):
        copy = pltpu.make_async_remote_copy(src_ref=src, dst_ref=dst, send_sem=send_sem.at[len(sends)], recv_sem=sem, device_id={'ep': target}, device_id_type=MESH)
        copy.start()
        sends.append(copy)

    def landed(ref, sem):
        pltpu.make_async_copy(ref, ref, sem).wait()

    def around(p, d):
        return (p + d) % RING

    other = 1 - c
    partner = dev(x, y, other)
    barrier = pltpu.get_barrier_semaphore()
    greet = [partner]
    for d in range(1, RING):
        greet += [dev(around(x, d), y, c), dev(around(x, d), y, other), dev(x, around(y, d), c), dev(x, around(y, d), other)]
    for target in greet:
        pl.semaphore_signal(barrier, inc=1, device_id={'ep': target}, device_id_type=MESH)

    loads = [pltpu.make_async_copy(s, d, w_sem.at[i]) for i, (s, d) in enumerate(((wg_hbm, wg), (wu_hbm, wu), (wd_hbm, wd)))]
    for load in loads:
        load.start()
    pl.semaphore_wait(barrier, len(greet))

    near = (1, 3, 2)
    own = [h2.at[:, pl.ds(0, half)], h2.at[:, pl.ds(half, half)]]

    def slot(part, py, pc, px):
        return hid.at[part, py, pc, px], h_sem.at[part, py, pc, px]

    for first in (True, False):
        for d in near:
            part_x, part_y = (0, 1) if first else (1, 0)
            push(own[part_x], *slot(part_x, y, c, x), dev(around(x, d), y, c))
            push(own[part_y], *slot(part_y, y, c, x), dev(x, around(y, d), c))
            if first:
                push(marks, tok.at[y, c, x], t_sem.at[y, c, x], dev(around(x, d), y, c))
                push(marks, tok.at[y, c, x], t_sem.at[y, c, x], dev(x, around(y, d), c))
        if first:
            push(own[0], *slot(0, y, c, x), partner)
            push(own[1], *slot(1, y, c, x), partner)
            push(marks, tok.at[y, c, x], t_sem.at[y, c, x], partner)
    for d in near:
        push(gate_b.at[around(x, d)], gat_b.at[x], gb_sem.at[x], dev(around(x, d), y, c))
        push(gate_a.at[around(y, d)], gat_a.at[y], ga_sem.at[y], dev(x, around(y, d), c))
    hid[0, y, c, x] = h2[:, :half]
    hid[1, y, c, x] = h2[:, half:]
    tok[y, c, x] = marks[...]
    gat_a[y] = gate_a[y]
    gat_b[x] = gate_b[x]

    late = []
    for d in near:
        px, py = around(x, d), around(y, d)
        for part, sy, sx in ((0, y, px), (1, py, x)):
            ref, sem = slot(part, sy, c, sx)
            landed(ref, sem)
            for e in near:
                target = dev(x, around(y, e), c) if part == 0 else dev(around(x, e), y, c)
                if e == 2:
                    late.append((ref, sem, target))
                else:
                    push(ref, ref, sem, target)
            push(ref, ref, sem, partner)
        ref, sem = tok.at[y, c, px], t_sem.at[y, c, px]
        landed(ref, sem)
        for e in near:
            push(ref, ref, sem, dev(x, around(y, e), c))
        push(ref, ref, sem, partner)
    for item in late:
        push(item[0], item[0], item[1], item[2])
    for d in near:
        px, py = around(x, d), around(y, d)
        for part, sy, sx in ((1, y, px), (0, py, x)):
            ref, sem = slot(part, sy, c, sx)
            landed(ref, sem)
            push(ref, ref, sem, partner)

    lane = iota((8, 128), 1)
    strict = jnp.where((iota((128, 128), 0) < iota((128, 128), 1)) & (iota((128, 128), 0) // rows == iota((128, 128), 1) // rows), 1.0, 0.0).astype(BF16)
    quad_seats = RING * seats

    def expert_chunk(step, py):
        keep = [[], []]
        for pc in range(CORES):
            ids = tok[py, pc, 0] + tok[py, pc, 1] + tok[py, pc, 2] + tok[py, pc, 3]
            hits = []
            for e in range(2):
                match = jnp.where(ids == (me * 2 + e + 1).astype(F32), 1.0, 0.0)
                hits.append(jnp.broadcast_to(jnp.sum(match, axis=0, keepdims=True), (8, 128)))
            rank = dot32((hits[0] + hits[1]).astype(BF16), strict)
            seat = rank + (lane // rows * seats).astype(F32)
            picks = []
            for e in range(2):
                pick = jnp.where((iota((quad_seats, 128), 0).astype(F32) == seat[0:1]) & (hits[e][0:1] > 0.5), 1.0, 0.0)
                keep[e].append(jnp.sum(pick, axis=1, keepdims=True))
                picks.append(pick.astype(BF16))
            pick = jnp.concatenate(picks, axis=0)
            for part in range(2):
                src = hid[part, py, pc].reshape(RING * rows, half)
                got = dot32(pick, src).astype(BF16)
                for e in range(2):
                    xs[e, pc * quad_seats:(pc + 1) * quad_seats, part * half:(part + 1) * half] = got[e * quad_seats:(e + 1) * quad_seats]
        if step == 0:
            loads[0].wait()
            loads[1].wait()
        hidden = []
        block = ff // 2
        for n in range(2):
            cols = slice(n * block, (n + 1) * block)
            a = dot32(xs[0], wg[0, :, cols]) + dot32(xs[1], wg[1, :, cols])
            u = dot32(xs[0], wu[0, :, cols]) + dot32(xs[1], wu[1, :, cols])
            hidden.append((jax.nn.silu(a) * u).astype(BF16))
        act = jnp.concatenate(hidden, axis=1)
        masks = [jnp.concatenate(k, axis=0) for k in keep]
        acts = [jnp.where(m > 0.5, act, jnp.zeros_like(act)) for m in masks]
        if step == 0:
            loads[2].wait()
        for n in range(4):
            cols = slice(n * half // 2, (n + 1) * half // 2)
            ys[step, :, cols] = (dot32(acts[0], wd[0, :, cols]) + dot32(acts[1], wd[1, :, cols])).astype(BF16)

    def first_leg(step, off):
        py = around(y, off)
        mine = CORES * x + c
        for dx in (0,) + near:
            for dc in range(CORES):
                px, pc = around(x, dx), (c + dc) % CORES
                src = ys.at[step, pl.ds((pc * RING + px) * seats, seats), pl.ds(0, half)]
                if dx == 0 and dc == 0:
                    r1a[py, mine] = src[...]
                else:
                    push(src, r1a.at[py, mine], r1a_sem.at[py, mine], dev(px, y, pc))
        for dc in range(CORES):
            pc = (c + dc) % CORES
            src = ys.at[step, pl.ds(pc * quad_seats, quad_seats), pl.ds(half, half)]
            if off == 0 and dc == 0:
                r1b[CORES * y + c] = src[...]
            else:
                push(src, r1b.at[CORES * y + c], r1b_sem.at[CORES * y + c], dev(x, py, pc))

    def weigh(gate, data):
        total = dot32(jnp.concatenate(split3(gate), axis=0), data)
        return total[:rows] + total[rows:2 * rows] + total[2 * rows:]

    def second_leg_a(off):
        py = around(y, off)
        for dx in (0,) + near:
            for dc in range(CORES):
                if dx or dc:
                    k = CORES * around(x, dx) + (c + dc) % CORES
                    landed(r1a.at[py, k], r1a_sem.at[py, k])
        if off:
            landed(gat_a.at[py], ga_sem.at[py])
        part = weigh(gat_a[py], r1a[py].reshape(RING * CORES * seats, half))
        if off:
            sa[py] = part
            push(sa.at[py], r2a.at[y], r2a_sem.at[y], dev(x, py, c))
        else:
            r2a[y] = part

    order = (0,) + near
    for step, off in enumerate(order):
        py = around(y, off)
        if step == 1:
            for d in near:
                qy = around(y, d)
                for e in near:
                    qx = around(x, e)
                    for part in range(2):
                        landed(*slot(part, qy, c, qx))
                        push(slot(part, qy, c, qx)[0], *slot(part, qy, c, qx), partner)
                for px in range(RING):
                    qx = around(x, px)
                    landed(tok.at[qy, c, qx], t_sem.at[qy, c, qx])
                    push(tok.at[qy, c, qx], tok.at[qy, c, qx], t_sem.at[qy, c, qx], partner)
        for px in range(RING):
            for part in range(2):
                landed(*slot(part, py, other, px))
            landed(tok.at[py, other, px], t_sem.at[py, other, px])
        expert_chunk(step, py)
        first_leg(step, off)
        if step:
            second_leg_a(order[step - 1])
    for d in near:
        for dc in range(CORES):
            k = CORES * around(y, d) + (c + dc) % CORES
            landed(r1b.at[k], r1b_sem.at[k])
    landed(r1b.at[CORES * y + other], r1b_sem.at[CORES * y + other])
    for d in near + (0,):
        px = around(x, d)
        if d:
            landed(gat_b.at[px], gb_sem.at[px])
        data = jnp.concatenate([r1b[k, pl.ds(px * seats, seats), :] for k in range(RING * CORES)], axis=0)
        part = weigh(gat_b[px], data)
        if d:
            sb[px] = part
            push(sb.at[px], r2b.at[x], r2b_sem.at[x], dev(px, y, c))
        else:
            r2b[x] = part
    second_leg_a(order[-1])
    for d in near:
        landed(r2a.at[around(y, d)], r2a_sem.at[around(y, d)])
    out[:, :half] = (x_mid[:, :half].astype(F32) + ((r2a[0] + r2a[1]) + (r2a[2] + r2a[3]))).astype(BF16)
    for d in near:
        landed(r2b.at[around(x, d)], r2b_sem.at[around(x, d)])
    out[:, half:] = (x_mid[:, half:].astype(F32) + ((r2b[0] + r2b[1]) + (r2b[2] + r2b[3]))).astype(BF16)
    for copy in sends:
        copy.wait_send()


def exchange(h2, marks, gate_a, gate_b, x_mid, w_gate, w_up, w_down, seats):
    rows, width = h2.shape
    half = width // 2
    e_local, _, ff = w_gate.shape
    line = RING * CORES
    vmem = pl.BlockSpec(memory_space=pltpu.VMEM)
    hbm = pl.BlockSpec(memory_space=pl.ANY)
    dma = pltpu.SemaphoreType.DMA
    return pl.pallas_call(
        exchange_kernel,
        out_shape=jax.ShapeDtypeStruct((rows, width), BF16),
        in_specs=[vmem] * 5 + [hbm] * 3,
        out_specs=vmem,
        scratch_shapes=[
            pltpu.VMEM((2, RING, CORES, RING, rows, half), BF16),
            pltpu.VMEM((RING, CORES, RING, 8, 128), F32),
            pltpu.VMEM((RING, rows, 128), F32),
            pltpu.VMEM((RING, rows, 128), F32),
            pltpu.VMEM(w_gate.shape, BF16),
            pltpu.VMEM(w_up.shape, BF16),
            pltpu.VMEM(w_down.shape, BF16),
            pltpu.VMEM((e_local, line * seats, width), BF16),
            pltpu.VMEM((RING, line * seats, width), BF16),
            pltpu.VMEM((RING, line, seats, half), BF16),
            pltpu.VMEM((line, RING * seats, half), BF16),
            pltpu.VMEM((RING, rows, half), F32),
            pltpu.VMEM((RING, rows, half), F32),
            pltpu.VMEM((RING, rows, half), F32),
            pltpu.VMEM((RING, rows, half), F32),
            dma((3,)),
            dma((2, RING, CORES, RING)),
            dma((RING, CORES, RING)),
            dma((RING,)),
            dma((RING,)),
            dma((RING, line)),
            dma((line,)),
            dma((RING,)),
            dma((RING,)),
            dma((192,)),
        ],
        compiler_params=pltpu.CompilerParams(collective_id=0, has_side_effects=True, vmem_limit_bytes=60 * 2 ** 20),
        name='exchange',
    )(h2, marks, gate_a, gate_b, x_mid, w_gate, w_up, w_down)


def solution(mesh):
    row_spec = P(('dp', 'ep'))
    rep = P()
    expert_spec = P('ep')
    in_specs = (row_spec,) * 5 + (rep,) * 9 + (expert_spec,) * 3

    def device_step(x_in, k_cache, v_cache, cache_len, topk_idx, ln_attn, w_q, w_k, w_v, q_norm, k_norm, w_o, ln_moe, w_router, w_gate, w_up, w_down):
        x_mid, k_full, v_full = attend_block(x_in, k_cache, v_cache, cache_len, ln_attn, w_q, w_k, w_v, q_norm, k_norm, w_o)
        rows, top_k = topk_idx.shape
        seats = 2 * rows * top_k // mesh.shape['ep']
        h2, gate_a, gate_b, marks = route(x_mid, topk_idx, ln_moe, w_router)
        x_out = exchange(h2, marks, gate_a, gate_b, x_mid, w_gate, w_up, w_down, seats)
        return x_out, k_full, v_full

    return jax.shard_map(device_step, mesh=mesh, in_specs=in_specs, out_specs=(row_spec,) * 3, check_vma=False)
```

```python
import functools
import math

import jax
import jax.numpy as jnp
from jax import lax
from jax.experimental import pallas as pl
from jax.experimental.pallas import tpu as pltpu
from jax.sharding import PartitionSpec as P

ROPE_BASE = 1000000.0
NORM_EPS = 1e-6
NEG = -1e30
RING = 4
CORES = 2
MESH = pl.DeviceIdType.MESH
F32 = jnp.float32
BF16 = jnp.bfloat16


def iota(shape, axis):
    return lax.broadcasted_iota(jnp.int32, shape, axis)


def split3(value):
    top = value.astype(BF16)
    rest = value - top.astype(F32)
    mid = rest.astype(BF16)
    low = (rest - mid.astype(F32)).astype(BF16)
    return top, mid, low


def dot32(lhs, rhs):
    return jnp.dot(lhs, rhs, preferred_element_type=F32)


def rms_rows(values, gain):
    return values * lax.rsqrt(jnp.mean(values * values, axis=-1, keepdims=True) + NORM_EPS) * gain


def choice_tables(topk_t, experts, x_pos):
    top_k, rows = topk_t.shape
    devs = RING * RING * CORES
    e_local = experts // devs
    seats = 2 * rows * top_k // devs
    lanes = devs * seats
    topk_b = (topk_t + 1).astype(F32).astype(BF16)
    eye = jnp.where(iota((top_k, 128), 0) == iota((top_k, 128), 1), 1.0, 0.0).astype(BF16)
    topk = lax.dot_general(topk_b, eye, (((0,), (0,)), ((), ())), preferred_element_type=F32)
    expert_ids = (iota((rows, experts), 1) + 1).astype(F32)
    hit = jnp.zeros((rows, experts), F32)
    for k in range(top_k):
        hit = hit + jnp.where(topk[:, k:k + 1] == expert_ids, 1.0, 0.0)
    before = jnp.where(iota((rows, rows), 1) < iota((rows, rows), 0), 1.0, 0.0).astype(BF16)
    seat_l = (iota((rows, lanes), 1) % seats).astype(F32)
    tables = []
    for by_row in (True, False):
        hit_l = dot32(hit.astype(BF16), spread_matrix(experts, lanes, seats, e_local, by_row))
        rank_l = dot32(before, hit_l.astype(BF16))
        tables.append(jnp.where(rank_l == seat_l, hit_l, 0.0))
    place = jnp.where(iota((rows, 128), 1) == x_pos * rows + iota((rows, 128), 0), 1.0, 0.0).astype(BF16)
    return hit, tables[0], tables[1], dot32(topk_b, place)


def flat_row(value):
    return jnp.concatenate([value[i:i + 1] for i in range(value.shape[0])], axis=1)


def spread_matrix(experts, lanes, seats, e_local, by_row):
    lane_dev = iota((experts, lanes), 1) // seats
    if not by_row:
        lane_dev = (lane_dev % (RING * CORES)) // CORES * (RING * CORES) + lane_dev // (RING * CORES) * CORES + lane_dev % CORES
    return jnp.where(iota((experts, lanes), 0) // e_local == lane_dev, 1.0, 0.0).astype(BF16)


def attend_kernel(lens, x_in, topk_t, ln_attn, q_norm, k_norm, ln_moe, w_router_t, k_hbm, v_hbm, wq_hbm, wk_hbm, wv_hbm, wo_hbm,
                  k_out, v_out, x_mid, h2, gate_a, gate_b, marks, kbuf, vbuf, wq, wk, wv, wo, raw, q_s, k_s, v_s, o_s, xm_s, hit_s, tab_a, tab_b,
                  w_sem, c_sem, out_sem):
    rows, width = x_in.shape
    slots, heads, hd = kbuf.shape[1:]
    experts = w_router_t.shape[0]
    blk = 2 * hd
    n_blk = width // blk
    group = 8
    n_grp = rows // group
    ahead = 4

    def w_copy(i, which):
        src, dst = ((wq_hbm, wq), (wk_hbm, wk), (wv_hbm, wv), (wo_hbm, wo))[which]
        return pltpu.make_async_copy(src.at[:, pl.ds(pl.multiple_of(i * blk, blk), blk)], dst.at[i], w_sem.at[which, i])

    def c_copy(g, which):
        src, dst = ((k_hbm, kbuf), (v_hbm, vbuf))[which]
        return pltpu.make_async_copy(src.at[pl.ds(g * group, group)], dst.at[pl.ds(g * group, group)], c_sem.at[which, g])

    def o_copy(g, which):
        src, dst = ((kbuf, k_out), (vbuf, v_out))[which]
        return pltpu.make_async_copy(src.at[pl.ds(g * group, group)], dst.at[pl.ds(g * group, group)], out_sem.at[which, g])

    for i in range(ahead):
        for which in range(3):
            w_copy(i, which).start()

    hit, one, two, mark = choice_tables(topk_t[...], experts, lax.axis_index('ep') // CORES % RING)
    hit_s[...] = hit
    tab_a[...] = one
    tab_b[...] = two
    marks[...] = mark

    row = iota((rows, hd), 0)
    lane = iota((rows, hd), 1)
    pos = jnp.zeros((rows, hd), F32)
    for b in range(rows):
        pos = jnp.where(row == b, lens[b].astype(F32), pos)
    half = hd // 2
    freq = jnp.exp((lane % half).astype(F32) * (-2.0 * math.log(ROPE_BASE) / hd))
    cosine = jnp.cos(pos * freq)
    sine = jnp.where(lane < half, -1.0, 1.0) * jnp.sin(pos * freq)
    q_gain = jnp.broadcast_to(q_norm[...].astype(F32), (rows, hd))
    k_gain = jnp.broadcast_to(k_norm[...].astype(F32), (rows, hd))
    normed = rms_rows(x_in[...].astype(F32), flat_row(ln_attn[...].astype(F32))).astype(BF16)

    def turn(value, gain):
        value = rms_rows(value, gain)
        return value * cosine + pltpu.roll(value, half, 1) * sine

    later = [functools.partial(c_copy, g, which) for g in range(n_grp) for which in range(2)] + [functools.partial(w_copy, i, 3) for i in range(n_blk)]
    for i in range(n_blk + 1):
        if i + ahead < n_blk:
            for which in range(3):
                w_copy(i + ahead, which).start()
        elif later:
            for copy in later[:4]:
                copy().start()
            later = later[4:]
        if i < n_blk:
            for which, buf in enumerate((wq, wk, wv)):
                w_copy(i, which).wait()
            for which, buf in enumerate((wq, wk, wv)):
                raw[i % 2, which] = dot32(normed, buf[i])
        if i:
            for s in range(2):
                dst = pl.ds(2 * (i - 1) + s, rows, stride=heads)
                cols = slice(s * hd, (s + 1) * hd)
                q_s[dst, :] = turn(raw[(i - 1) % 2, 0, :, cols], q_gain)
                k_s[dst, :] = turn(raw[(i - 1) % 2, 1, :, cols], k_gain)
                v_s[dst, :] = raw[(i - 1) % 2, 2, :, cols]
    for copy in later:
        copy().start()

    key = iota((heads, slots * heads), 1)
    same = key % heads == iota((heads, slots * heads), 0)
    scale = hd ** -0.5

    def one_group(g, carry):
        c_copy(g, 0).wait()
        c_copy(g, 1).wait()
        scores = []
        for i in range(group):
            b = g * group + i
            at = pl.ds(pl.multiple_of(b * heads, heads), heads)
            length = lens[b]
            k_row = k_s[at, :].astype(BF16)
            v_row = v_s[at, :].astype(BF16)
            kbuf[b, length] = k_row
            vbuf[b, length] = v_row
            keys = kbuf[b].reshape(slots * heads, hd)
            score = lax.dot_general(q_s[at, :].astype(BF16), keys, (((1,), (1,)), ((), ())), preferred_element_type=F32) * scale
            scores.append(jnp.where(same & (key // heads <= length), score, NEG))
        for i in range(group):
            b = g * group + i
            raw = jnp.exp(scores[i] - jnp.max(scores[i], axis=1, keepdims=True))
            prob = (raw / jnp.sum(raw, axis=1, keepdims=True)).astype(BF16)
            mixed = dot32(prob, vbuf[b].reshape(slots * heads, hd))
            o_s[pl.ds(pl.multiple_of(b * heads, heads), heads), :] = mixed
        return carry

    lax.fori_loop(0, n_grp, one_group, 0)
    att = jnp.concatenate([o_s[pl.ds(h, rows, stride=heads), :].astype(BF16) for h in range(heads)], axis=1)
    for i in range(n_blk):
        w_copy(i, 3).wait()
        if i >= n_blk - n_grp:
            o_copy(i - n_blk + n_grp, 0).start()
            o_copy(i - n_blk + n_grp, 1).start()
        cols = slice(i * blk, (i + 1) * blk)
        xm_s[:, cols] = (x_in[:, cols].astype(F32) + dot32(att, wo[i])).astype(BF16)
    mid = xm_s[...]
    x_mid[...] = mid
    h_moe = rms_rows(mid.astype(F32), flat_row(ln_moe[...].astype(F32))).astype(BF16)
    h2[...] = h_moe
    logits = lax.dot_general(h_moe, w_router_t[...], (((1,), (1,)), ((), ())), preferred_element_type=F32)
    chosen = hit_s[...] > 0.5
    peak = jnp.max(jnp.where(chosen, logits, NEG), axis=1, keepdims=True)
    raw = jnp.where(chosen, jnp.exp(jnp.where(chosen, logits, peak) - peak), 0.0)
    parts = split3(raw / jnp.sum(raw, axis=1, keepdims=True))
    lanes = tab_a.shape[1]
    devs = RING * RING * CORES
    for by_row, table, dst in ((True, tab_a, gate_a), (False, tab_b, gate_b)):
        spread = spread_matrix(experts, lanes, lanes // devs, experts // devs, by_row)
        gate = (dot32(parts[0], spread) + dot32(parts[1], spread) + dot32(parts[2], spread)) * table[...]
        for i in range(RING):
            dst[i] = gate[:, i * 128:(i + 1) * 128]
    for g in range(n_grp):
        o_copy(g, 0).wait()
        o_copy(g, 1).wait()


def attend(x_in, k_cache, v_cache, cache_len, topk, ln_attn, w_q, w_k, w_v, q_norm, k_norm, w_o, ln_moe, w_router):
    rows, slots, heads, hd = k_cache.shape
    width = x_in.shape[1]
    experts = w_router.shape[1]
    lanes = 2 * rows * topk.shape[1]
    n_blk = width // (2 * hd)
    vmem = pl.BlockSpec(memory_space=pltpu.VMEM)
    hbm = pl.BlockSpec(memory_space=pl.ANY)
    dma = pltpu.SemaphoreType.DMA
    weight = pltpu.VMEM((n_blk, width, 2 * hd), BF16)
    return pl.pallas_call(
        attend_kernel,
        out_shape=(
            jax.ShapeDtypeStruct(k_cache.shape, BF16),
            jax.ShapeDtypeStruct(v_cache.shape, BF16),
            jax.ShapeDtypeStruct((rows, width), BF16),
            jax.ShapeDtypeStruct((rows, width), BF16),
            jax.ShapeDtypeStruct((RING, rows, 128), F32),
            jax.ShapeDtypeStruct((RING, rows, 128), F32),
            jax.ShapeDtypeStruct((8, 128), F32),
        ),
        in_specs=[pl.BlockSpec(memory_space=pltpu.SMEM)] + [vmem] * 7 + [hbm] * 6,
        out_specs=[hbm, hbm] + [vmem] * 5,
        scratch_shapes=[
            pltpu.VMEM(k_cache.shape, BF16),
            pltpu.VMEM(v_cache.shape, BF16),
            weight, weight, weight, weight,
            pltpu.VMEM((2, 3, rows, 2 * hd), F32),
            pltpu.VMEM((rows * heads, hd), F32),
            pltpu.VMEM((rows * heads, hd), F32),
            pltpu.VMEM((rows * heads, hd), F32),
            pltpu.VMEM((rows * heads, hd), F32),
            pltpu.VMEM((rows, width), BF16),
            pltpu.VMEM((rows, experts), F32),
            pltpu.VMEM((rows, lanes), F32),
            pltpu.VMEM((rows, lanes), F32),
            dma((4, n_blk)),
            dma((2, rows // 8)),
            dma((2, rows // 8)),
        ],
        compiler_params=pltpu.CompilerParams(vmem_limit_bytes=60 * 2 ** 20),
        name='attend',
    )(cache_len, x_in, topk.T, ln_attn.reshape(width // 128, 128), q_norm.reshape(1, hd), k_norm.reshape(1, hd), ln_moe.reshape(width // 128, 128), w_router.T, k_cache, v_cache, w_q, w_k, w_v, w_o)


def exchange_kernel(h2, marks, gate_a, gate_b, x_mid, wg_hbm, wu_hbm, wd_hbm, out, hid, tok, gat, wg, wu, wd, xs, ys, r1a, r1b, sa, sb, r2a, r2b,
                    w_sem, h_sem, hp_sem, t_sem, tp_sem, g_sem, r1a_sem, r1b_sem, r2_sem, send_sem):
    rows, width = h2.shape
    half = width // 2
    cut = r1a.shape[2]
    rest = width - cut
    seats = r1a.shape[1]
    ff = wg.shape[2]
    me = lax.axis_index('ep')
    c = me % CORES
    x = me // CORES % RING
    y = me // (CORES * RING)
    sent = [0] * 8

    def dev(px, py, pc):
        return (py * RING + px) * CORES + pc

    def push(kind, src, dst, sem, target):
        pltpu.make_async_remote_copy(src_ref=src, dst_ref=dst, send_sem=send_sem.at[kind], recv_sem=sem, device_id={'ep': target}, device_id_type=MESH).start()
        sent[kind] += 1

    def landed(ref, sem):
        pltpu.make_async_copy(ref, ref, sem).wait()

    def around(p, d):
        return (p + d) % RING

    other = 1 - c
    partner = dev(x, y, other)
    barrier = pltpu.get_barrier_semaphore()
    greet = [partner]
    for d in range(1, RING):
        greet += [dev(around(x, d), y, c), dev(around(x, d), y, other), dev(x, around(y, d), c), dev(x, around(y, d), other)]
    for target in greet:
        pl.semaphore_signal(barrier, inc=1, device_id={'ep': target}, device_id_type=MESH)

    loads = [pltpu.make_async_copy(s, d, w_sem.at[i]) for i, (s, d) in enumerate(((wg_hbm, wg), (wu_hbm, wu), (wd_hbm, wd)))]
    for load in loads:
        load.start()
    pl.semaphore_wait(barrier, len(greet))

    near = (1, 3, 2)

    def block_at(part, py, pc, px):
        return ((part * RING + py) * CORES + pc) * RING + px

    def slot(part, py, px):
        return hid.at[block_at(part, py, c, px)], h_sem.at[part, py, px]

    def mark_at(py, pc, px):
        return (py * CORES + pc) * RING + px

    def to_partner(part, py, px):
        ref = hid.at[block_at(part, py, c, px)]
        push(0, ref, ref, hp_sem.at[part, py], partner)

    own = [h2.at[:, pl.ds(0, half)], h2.at[:, pl.ds(half, half)]]
    my_mark = tok.at[mark_at(y, c, x)]
    for first in (True, False):
        part_x, part_y = (0, 1) if first else (1, 0)
        for d in near:
            push(0, own[part_x], *slot(part_x, y, x), dev(around(x, d), y, c))
            push(0, own[part_y], *slot(part_y, y, x), dev(x, around(y, d), c))
        if first:
            for d in near:
                push(2, marks, my_mark, t_sem.at[y, x], dev(around(x, d), y, c))
                push(2, marks, my_mark, t_sem.at[y, x], dev(x, around(y, d), c))
            push(0, own[0], hid.at[block_at(0, y, c, x)], hp_sem.at[0, y], partner)
            push(0, own[1], hid.at[block_at(1, y, c, x)], hp_sem.at[1, y], partner)
            push(2, marks, my_mark, tp_sem.at[y], partner)
    for d in near:
        push(3, gate_b.at[around(x, d)], gat.at[RING + x], g_sem.at[1], dev(around(x, d), y, c))
        push(3, gate_a.at[around(y, d)], gat.at[y], g_sem.at[0], dev(x, around(y, d), c))
    hid[block_at(0, y, c, x)] = h2[:, :half]
    hid[block_at(1, y, c, x)] = h2[:, half:]
    tok[mark_at(y, c, x)] = marks[...]
    gat[y] = gate_a[y]
    gat[RING + x] = gate_b[x]

    def onward(part, py, px, steps):
        ref, sem = slot(part, py, px)
        for e in steps:
            push(0, ref, ref, sem, dev(x, around(y, e), c) if part == 0 else dev(around(x, e), y, c))

    for d in near:
        px, py = around(x, d), around(y, d)
        landed(*slot(0, y, px))
        onward(0, y, px, (1, 3))
        to_partner(0, y, px)
        landed(*slot(1, py, x))
        onward(1, py, x, (1, 3))
        to_partner(1, py, x)
        ref = tok.at[mark_at(y, c, px)]
        landed(ref, t_sem.at[y, px])
        for e in near:
            push(2, ref, ref, t_sem.at[y, px], dev(x, around(y, e), c))
        push(2, ref, ref, tp_sem.at[y], partner)
    for d in near:
        onward(0, y, around(x, d), (2,))
        onward(1, around(y, d), x, (2,))
    for d in near:
        px, py = around(x, d), around(y, d)
        landed(*slot(1, y, px))
        to_partner(1, y, px)
        landed(*slot(0, py, x))
        to_partner(0, py, x)

    lane = iota((8, 128), 1)
    strict = jnp.where((iota((128, 128), 0) < iota((128, 128), 1)) & (iota((128, 128), 0) // rows == iota((128, 128), 1) // rows), 1.0, 0.0).astype(BF16)
    quad_seats = RING * seats

    def expert_chunk(step, quads):
        keep = [[], []]
        for q, (off, dc) in enumerate(quads):
            py, pc = around(y, off), (c + dc) % CORES
            first = mark_at(py, pc, 0)
            ids = tok[first] + tok[first + 1] + tok[first + 2] + tok[first + 3]
            hits = []
            for e in range(2):
                match = jnp.where(ids == (me * 2 + e + 1).astype(F32), 1.0, 0.0)
                hits.append(jnp.broadcast_to(jnp.sum(match, axis=0, keepdims=True), (8, 128)))
            rank = dot32((hits[0] + hits[1]).astype(BF16), strict)
            seat = rank + (lane // rows * seats).astype(F32)
            picks = []
            for e in range(2):
                pick = jnp.where((iota((quad_seats, 128), 0).astype(F32) == seat[0:1]) & (hits[e][0:1] > 0.5), 1.0, 0.0)
                keep[e].append(jnp.sum(pick, axis=1, keepdims=True))
                picks.append(pick.astype(BF16))
            pick = jnp.concatenate(picks, axis=0)
            for part in range(2):
                src = hid[pl.ds(block_at(part, py, pc, 0), RING)].reshape(RING * rows, half)
                got = dot32(pick, src).astype(BF16)
                for e in range(2):
                    xs[e, q * quad_seats:(q + 1) * quad_seats, part * half:(part + 1) * half] = got[e * quad_seats:(e + 1) * quad_seats]
        if step == 0:
            loads[0].wait()
            loads[1].wait()
        hidden = []
        block = ff // 2
        for n in range(2):
            cols = slice(n * block, (n + 1) * block)
            a = dot32(xs[0], wg[0, :, cols]) + dot32(xs[1], wg[1, :, cols])
            u = dot32(xs[0], wu[0, :, cols]) + dot32(xs[1], wu[1, :, cols])
            hidden.append((jax.nn.silu(a) * u).astype(BF16))
        act = jnp.concatenate(hidden, axis=1)
        masks = [jnp.concatenate(k, axis=0) for k in keep]
        acts = [jnp.where(m > 0.5, act, jnp.zeros_like(act)) for m in masks]
        if step == 0:
            loads[2].wait()
        for lo, leg in ((half, leg_b), (0, leg_a)):
            for at in range(lo, lo + half, half // 2):
                cols = slice(at, at + half // 2)
                ys[step, :, cols] = (dot32(acts[0], wd[0, :, cols]) + dot32(acts[1], wd[1, :, cols])).astype(BF16)
            for q, (off, dc) in enumerate(quads):
                leg(step, q, off, dc)

    def leg_a(step, q, off, dc):
        py, pc = around(y, off), (c + dc) % CORES
        mine = CORES * x + c
        for dx in (0,) + near:
            px = around(x, dx)
            src = ys.at[step, pl.ds(q * quad_seats + px * seats, seats), pl.ds(0, cut)]
            if dx == 0 and dc == 0:
                r1a[py * RING * CORES + mine] = src[...]
            else:
                push(4, src, r1a.at[py * RING * CORES + mine], r1a_sem.at[py], dev(px, y, pc))

    def leg_b(step, q, off, dc):
        mine = CORES * y + c
        src = ys.at[step, pl.ds(q * quad_seats, quad_seats), pl.ds(cut, rest)]
        if off == 0 and dc == 0:
            r1b[mine] = src[...]
        else:
            push(5, src, r1b.at[mine], r1b_sem.at[0], dev(x, around(y, off), (c + dc) % CORES))

    def weigh(gate, data):
        total = dot32(jnp.concatenate(split3(gate), axis=0), data)
        return total[:rows] + total[rows:2 * rows] + total[2 * rows:]

    def second_leg_a(off):
        py = around(y, off)
        line = RING * CORES
        landed(r1a.at[pl.ds(py * line, line - 1)], r1a_sem.at[py])
        part = weigh(gat[py], r1a[pl.ds(py * line, line)].reshape(line * seats, cut))
        if off:
            sa[py] = part
            push(6, sa.at[py], r2a.at[y], r2_sem.at[0], dev(x, py, c))
        else:
            r2a[y] = part

    def share_row(d):
        qy = around(y, d)
        for e in near:
            qx = around(x, e)
            landed(*slot(0, qy, qx))
            to_partner(0, qy, qx)
            landed(*slot(1, qy, qx))
            to_partner(1, qy, qx)
        for e in range(RING):
            qx = around(x, e)
            ref = tok.at[mark_at(qy, c, qx)]
            landed(ref, t_sem.at[qy, qx])
            push(2, ref, ref, tp_sem.at[qy], partner)

    def partner_row(d):
        qy = around(y, d)
        for part in range(2):
            landed(hid.at[pl.ds(block_at(part, qy, other, 0), RING)], hp_sem.at[part, qy])
        landed(tok.at[pl.ds(mark_at(qy, other, 0), RING)], tp_sem.at[qy])

    partner_row(0)
    expert_chunk(0, ((0, 0), (0, 1)))
    share_row(1)
    share_row(3)
    expert_chunk(1, ((1, 0), (3, 0)))
    share_row(2)
    landed(gat.at[pl.ds(0, RING - 1)], g_sem.at[0])
    landed(gat.at[pl.ds(0, RING - 1)], g_sem.at[1])
    second_leg_a(0)
    partner_row(2)
    expert_chunk(2, ((2, 0), (2, 1)))
    partner_row(1)
    partner_row(3)
    expert_chunk(3, ((1, 1), (3, 1)))
    second_leg_a(2)
    landed(r1b.at[pl.ds(0, RING * CORES - 1)], r1b_sem.at[0])
    for d in (2, 1, 3, 0):
        px = around(x, d)
        data = jnp.concatenate([r1b[k, pl.ds(px * seats, seats), :] for k in range(RING * CORES)], axis=0)
        part = weigh(gat[RING + px], data)
        if d:
            sb[px] = part
            push(7, sb.at[px], r2b.at[x], r2_sem.at[1], dev(px, y, c))
        else:
            r2b[x] = part
    second_leg_a(1)
    second_leg_a(3)
    landed(r2a.at[pl.ds(0, RING - 1)], r2_sem.at[0])
    out[:, :cut] = (x_mid[:, :cut].astype(F32) + ((r2a[0] + r2a[1]) + (r2a[2] + r2a[3]))).astype(BF16)
    landed(r2b.at[pl.ds(0, RING - 1)], r2_sem.at[1])
    out[:, cut:] = (x_mid[:, cut:].astype(F32) + ((r2b[0] + r2b[1]) + (r2b[2] + r2b[3]))).astype(BF16)
    sizes = (hid, hid, tok, gat, r1a, r1b, r2a, r2b)
    for kind, ref in enumerate(sizes):
        if sent[kind]:
            landed(ref.at[pl.ds(0, sent[kind])], send_sem.at[kind])


def exchange(h2, marks, gate_a, gate_b, x_mid, w_gate, w_up, w_down, seats):
    rows, width = h2.shape
    half = width // 2
    cut = width * 5 // 8
    rest = width - cut
    e_local, _, ff = w_gate.shape
    line = RING * CORES
    vmem = pl.BlockSpec(memory_space=pltpu.VMEM)
    hbm = pl.BlockSpec(memory_space=pl.ANY)
    dma = pltpu.SemaphoreType.DMA
    return pl.pallas_call(
        exchange_kernel,
        out_shape=jax.ShapeDtypeStruct((rows, width), BF16),
        in_specs=[vmem] * 5 + [hbm] * 3,
        out_specs=vmem,
        scratch_shapes=[
            pltpu.VMEM((2 * RING * line, rows, half), BF16),
            pltpu.VMEM((RING * line, 8, 128), F32),
            pltpu.VMEM((2 * RING, rows, 128), F32),
            pltpu.VMEM(w_gate.shape, BF16),
            pltpu.VMEM(w_up.shape, BF16),
            pltpu.VMEM(w_down.shape, BF16),
            pltpu.VMEM((e_local, line * seats, width), BF16),
            pltpu.VMEM((RING, line * seats, width), BF16),
            pltpu.VMEM((RING * line, seats, cut), BF16),
            pltpu.VMEM((line, RING * seats, rest), BF16),
            pltpu.VMEM((RING, rows, cut), F32),
            pltpu.VMEM((RING, rows, rest), F32),
            pltpu.VMEM((RING, rows, cut), F32),
            pltpu.VMEM((RING, rows, rest), F32),
            dma((3,)),
            dma((2, RING, RING)),
            dma((2, RING)),
            dma((RING, RING)),
            dma((RING,)),
            dma((2,)),
            dma((RING,)),
            dma((1,)),
            dma((2,)),
            dma((8,)),
        ],
        compiler_params=pltpu.CompilerParams(collective_id=0, has_side_effects=True, vmem_limit_bytes=60 * 2 ** 20),
        name='exchange',
    )(h2, marks, gate_a, gate_b, x_mid, w_gate, w_up, w_down)


def solution(mesh):
    row_spec = P(('dp', 'ep'))
    rep = P()
    expert_spec = P('ep')
    in_specs = (row_spec,) * 5 + (rep,) * 9 + (expert_spec,) * 3

    def device_step(x_in, k_cache, v_cache, cache_len, topk_idx, ln_attn, w_q, w_k, w_v, q_norm, k_norm, w_o, ln_moe, w_router, w_gate, w_up, w_down):
        rows, top_k = topk_idx.shape
        seats = 2 * rows * top_k // mesh.shape['ep']
        k_full, v_full, x_mid, h2, gate_a, gate_b, marks = attend(x_in, k_cache, v_cache, cache_len, topk_idx, ln_attn, w_q, w_k, w_v, q_norm, k_norm, w_o, ln_moe, w_router)
        x_out = exchange(h2, marks, gate_a, gate_b, x_mid, w_gate, w_up, w_down, seats)
        return x_out, k_full, v_full

    return jax.shard_map(device_step, mesh=mesh, in_specs=in_specs, out_specs=(row_spec,) * 3, check_vma=False)
```
